32 devices in a mesh: ctx: 8 (over z, x), tp: 4 (over y, core).
Axes of the slice: x: 2, y: 2, z: 4, core: 2. Of those that a mesh axis runs over, the one named last changes fastest.
Arguments:
- queries: bfloat16 [2048, 8192], P('ctx', 'tp'), may hold values from -8 to 8
- keys: bfloat16 [2048, 1024], P('ctx'), may hold values from -7 to 7
- values: bfloat16 [2048, 1024], P('ctx'), may hold values from -6 to 6
- out_weight: bfloat16 [8192, 4096], P('tp'), may hold values from -0.25 to 0.25
- block_order: int32 [16], P('ctx'), may hold values from 0 to 15, each once
Outputs:
- projected: bfloat16 [2048, 4096], P('ctx', 'tp')
The draws below stay inside these ranges and needn't reach their ends.
Inputs may be any that keep to these rules, and one draw needn't show every extreme that they name: `block_order`: every sequence block appears exactly once.
All inputs are finite; a program needn't handle non-finite values.
Results may differ from the reference program's by a relative error of at most 0.015.
Values may be sent and summed in bfloat16 or wider, within the bound.
A program may use at most 64 MiB of HBM per device.

```python
import math
import jax
import jax.numpy as jnp
from jax import lax

QUERY_HEADS = 64
KEY_VALUE_HEADS = 8
HEAD_SIZE = 128
DW = 4096
BLK = 128
SEQUENCE_TOKENS = 2048
NBLK = 16


def shared_vectors(key):
    key_random_keys = jax.random.fold_in(key, 11)
    key_queries = jax.random.fold_in(key, 12)
    key_collection = jnp.clip(jax.random.normal(key_random_keys, (SEQUENCE_TOKENS, KEY_VALUE_HEADS * HEAD_SIZE), jnp.float32), -6.0, 6.0)
    queryset = jnp.clip(2.5 * jax.random.normal(key_queries, (SEQUENCE_TOKENS, QUERY_HEADS * HEAD_SIZE), jnp.float32), -8.0, 8.0)
    return (key_collection.astype(jnp.bfloat16), queryset.astype(jnp.bfloat16))


def draw_queries(key, part):
    return shared_vectors(key)[1]


def draw_keys(key, part):
    return shared_vectors(key)[0]


def steps_of(key, shape, split, least, largest):
    def one(dim, parts):
        heights = jax.random.uniform(jax.random.fold_in(jax.random.fold_in(key, 6), dim), (parts,), jnp.float32, least / len(split), largest / len(split))
        return jnp.repeat(jnp.exp(heights), shape[dim] // parts).reshape((-1,) + (1,) * (len(shape) - dim - 1))

    gain = one(*split[0])
    for cut in split[1:]:
        gain = gain * one(*cut)
    return gain


def noise(key, extent, deviation, bound, cuts=(), kind=jnp.bfloat16):
    drawn = jax.random.normal(key, extent, jnp.float32) * deviation
    if len(cuts) > 0:
        drawn = steps_of(key, extent, cuts, -0.22, 0.18) * drawn
    return jnp.clip(drawn, min=-bound, max=bound).astype(kind)


def setup_inputs(seed: int = 0) -> dict:
    key_list = jax.random.split(jax.random.key(seed), 6)
    return {
        "queries": draw_queries(jax.random.fold_in(key_list[5], 71), 0),
        "keys": draw_keys(jax.random.fold_in(key_list[5], 71), 0),
        "values": noise(key_list[2], (SEQUENCE_TOKENS, KEY_VALUE_HEADS * HEAD_SIZE), 1.0, 6.0, ((0, 8),)),
        "out_weight": noise(key_list[3], (QUERY_HEADS * HEAD_SIZE, DW), (QUERY_HEADS * HEAD_SIZE // 16) ** -0.5, 0.25, ((0, 4),)),
        "block_order": jax.random.permutation(key_list[4], NBLK).astype(jnp.int32),
    }


def reference(queries, keys, values, out_weight, block_order):
    head_group = QUERY_HEADS // KEY_VALUE_HEADS
    offsets = jnp.arange(BLK, dtype=jnp.int32)
    positions = (block_order[:, None].astype(jnp.int32) * BLK + offsets[None, :]).reshape(-1)
    scale = 1.0 / math.sqrt(HEAD_SIZE)
    q_heads = jnp.transpose(queries.reshape(SEQUENCE_TOKENS, QUERY_HEADS, HEAD_SIZE), (1, 0, 2))
    key_head_rows = jnp.transpose(keys.reshape(SEQUENCE_TOKENS, KEY_VALUE_HEADS, HEAD_SIZE), (1, 0, 2))
    value_head_rows = jnp.transpose(values.reshape(SEQUENCE_TOKENS, KEY_VALUE_HEADS, HEAD_SIZE), (1, 0, 2))
    q_pos = positions.reshape(SEQUENCE_TOKENS // BLK, BLK)

    def one_head(head):
        k_rows = key_head_rows[head // head_group]
        v_rows = value_head_rows[head // head_group]
        q_blocks = q_heads[head].reshape(SEQUENCE_TOKENS // BLK, BLK, HEAD_SIZE)

        def one_block(item):
            q_rows, rows_pos = item
            scores = jnp.dot(q_rows, k_rows.T, preferred_element_type=jnp.float32) * scale
            visible = positions[None, :] <= rows_pos[:, None]
            top = lax.optimization_barrier(jnp.max(jnp.where(visible, scores, -jnp.inf), axis=1, keepdims=True))
            weights = jnp.where(visible, jnp.exp(scores - top), 0.0)
            total = lax.optimization_barrier(jnp.sum(weights, axis=1, keepdims=True))
            return jnp.dot(weights.astype(jnp.bfloat16), v_rows, preferred_element_type=jnp.float32) / total
        return lax.map(one_block, (q_blocks, q_pos)).reshape(SEQUENCE_TOKENS, HEAD_SIZE)
    heads_out = lax.map(one_head, jnp.arange(QUERY_HEADS, dtype=jnp.int32))
    attended = jnp.transpose(heads_out, (1, 0, 2)).reshape(SEQUENCE_TOKENS, QUERY_HEADS * HEAD_SIZE).astype(jnp.bfloat16)
    return jnp.dot(attended, out_weight, preferred_element_type=jnp.float32).astype(jnp.bfloat16)
```

```python
import functools
import math

import jax
import jax.numpy as jnp
from jax import lax
from jax.experimental import pallas as pl
from jax.experimental.pallas import tpu as pltpu
from jax.sharding import PartitionSpec as P

QUERY_HEADS = 64
KEY_VALUE_HEADS = 8
HEAD_SIZE = 128
MESH = pl.DeviceIdType.MESH
NT = (((1,), (1,)), ((), ()))


def kernel(dims, q_hbm, k_hbm, v_hbm, w_hbm, order, o_ref, q, w, kv, tile, orders, mask, eye, scores,
           att, pair_out, pair_in, far_out, far_in, load_sem, order_send, order_recv, send, recv,
           pair_send, pair_recv, far_send, far_recv):
    n, tp, rows, heads, kv_heads, unit, wide = dims
    line, groups = n // 2, tp // 2
    tokens = n * rows
    blocks = rows // 128
    per_kv = heads // kv_heads
    me, t = lax.axis_index("ctx"), lax.axis_index("tp")
    a, b = me // 2, lax.rem(me, 2)
    y, c = t // 2, lax.rem(t, 2)
    other = 1 - b
    partner = (me, y * 2 + 1 - c)

    def far(i):
        return lax.rem(y + i, groups)

    first = t * heads // (QUERY_HEADS // KEY_VALUE_HEADS)
    own = pl.ds(pl.multiple_of(me * rows, 128), rows)
    loads = []
    for p in range(2 * kv_heads):
        src = v_hbm if p % 2 else k_hbm
        cols = pl.ds(pl.multiple_of((first + p // 2) * HEAD_SIZE, 128), HEAD_SIZE)
        loads.append(pltpu.make_async_copy(src.at[:, cols], kv.at[p, own, :], load_sem.at[p]))
        loads[-1].start()
    q_load = pltpu.make_async_copy(q_hbm, q, load_sem.at[2 * kv_heads])
    w_load = pltpu.make_async_copy(w_hbm, w, load_sem.at[2 * kv_heads + 1])
    q_load.start()
    w_load.start()
    for i in range(blocks):
        tile[pl.ds(i, 1), :] = jnp.full((1, 128), order[i], jnp.int32)

    barrier = pltpu.get_barrier_semaphore()
    for d in range(1, n):
        pl.semaphore_signal(barrier, inc=1, device_id=(lax.rem(me + d, n), t), device_id_type=MESH)
    pl.semaphore_signal(barrier, inc=1, device_id=partner, device_id_type=MESH)
    for i in range(1, groups):
        pl.semaphore_signal(barrier, inc=1, device_id=(me, far(i) * 2 + c), device_id_type=MESH)
    pl.semaphore_wait(barrier, n - 1 + 1 + groups - 1)

    def order_copy(d, src_dev, target):
        return pltpu.make_async_remote_copy(
            src_ref=tile, dst_ref=orders.at[src_dev], send_sem=order_send.at[d],
            recv_sem=order_recv.at[d], device_id=(target, t), device_id_type=MESH)

    def piece(p, block, way, target):
        at = pl.ds(pl.multiple_of(block * rows, 128), rows)
        return pltpu.make_async_remote_copy(
            src_ref=kv.at[p, at, :], dst_ref=kv.at[p, at, :], send_sem=send.at[p, block, way],
            recv_sem=recv.at[p, block], device_id=(target, t), device_id_type=MESH)

    def guarded(cond, act):
        pl.when(cond)(act)

    def open_line(p):
        guarded(a + 1 < line, lambda: piece(p, me, 0, me + 2).start())
        guarded(a > 0, lambda: piece(p, me, 1, me - 2).start())
        piece(p, me, 2, a * 2 + other).start()

    def open_crossed(p):
        blk = a * 2 + other
        piece(p, blk, 2, blk).wait_recv()
        guarded(a + 1 < line, lambda: piece(p, blk, 0, me + 2).start())
        guarded(a > 0, lambda: piece(p, blk, 1, me - 2).start())

    def relay(p, s, side, crossing):
        low, high = (a - s) * 2 + side, (a + s) * 2 + side

        @pl.when(a - s >= 0)
        def _():
            piece(p, low, 0, me).wait_recv()
            guarded(a + 1 < line, lambda: piece(p, low, 0, me + 2).start())
            if crossing:
                piece(p, low, 2, a * 2 + other).start()

        @pl.when(a + s < line)
        def _():
            piece(p, high, 1, me).wait_recv()
            guarded(a > 0, lambda: piece(p, high, 1, me - 2).start())
            if crossing:
                piece(p, high, 2, a * 2 + other).start()

    def step(h, s):
        relay(2 * h, s, b, True)
        relay(2 * h + 1, s, b, False)
        relay(2 * h + 1, s, other, False)

    def finish(h):
        def body(i, _):
            piece(2 * h, i * 2 + other, 2, me).wait_recv()
            return 0
        lax.fori_loop(0, line, body, 0)

    for h in range(kv_heads):
        for p in (2 * h, 2 * h + 1):
            loads[p].wait()
            open_line(p)
        if h == 0:
            for d in range(1, n):
                order_copy(d, me, lax.rem(me + d, n)).start()
    orders[pl.ds(me, 1)] = tile[...][None]
    row = lax.broadcasted_iota(jnp.int32, (128, 128), 0)
    col = lax.broadcasted_iota(jnp.int32, (128, 128), 1)
    eye[...] = (row == col).astype(jnp.bfloat16)
    open_crossed(1)

    for d in range(1, n):
        order_copy(d, lax.rem(me + n - d, n), me).wait_recv()

    def build(i, _):
        for j in range(blocks):
            kpos = orders[pl.ds(i, 1), j:j + 1, :][0] * 128 + row
            for g in range(blocks):
                qpos = tile[g:g + 1, :] * 128 + col
                at = pl.ds(pl.multiple_of(i * rows + j * 128, 128), 128)
                mask[g, at, :] = jnp.where(kpos <= qpos, 0.0, -1e30).astype(jnp.bfloat16)
        return 0
    lax.fori_loop(0, n, build, 0)

    for s in range(1, line):
        step(0, s)
    finish(0)
    q_load.wait()

    chunk = tokens // 4
    factor = math.log2(math.e) / math.sqrt(HEAD_SIZE)
    ones = jnp.ones((chunk, 128), jnp.bfloat16)
    per_block = per_kv // unit

    def attend(h, g, u):
        at = pl.ds(pl.multiple_of(g * 128, 128), 128)
        def head_cols(k):
            return pl.ds(pl.multiple_of((h * per_kv + u * unit + k) * HEAD_SIZE, 128), HEAD_SIZE)
        e = eye[...]
        qa = jnp.concatenate(
            [jnp.concatenate([q[at, head_cols(k)], e], axis=1) for k in range(unit)], axis=0)
        top = None
        for i in range(4):
            ks = pl.ds(i * chunk, chunk)
            ka = jnp.concatenate([kv[2 * h, ks, :], mask[g, ks, :]], axis=1)
            s = lax.dot_general(qa, ka, NT, preferred_element_type=jnp.float32)
            scores[:, ks] = s
            for j in range(0, chunk, 128):
                part = s[:, j:j + 128]
                top = part if top is None else jnp.maximum(top, part)
        top = jnp.max(top, axis=1, keepdims=True)
        acc = None
        for i in range(4):
            ks = pl.ds(i * chunk, chunk)
            weight = jnp.exp2((scores[:, ks] - top) * factor).astype(jnp.bfloat16)
            va = jnp.concatenate([kv[2 * h + 1, ks, :], ones], axis=1)
            part = jnp.dot(weight, va, preferred_element_type=jnp.float32)
            acc = part if acc is None else acc + part
        res = (acc[:, :128] / acc[:, 128:]).astype(jnp.bfloat16)
        for k in range(unit):
            att[at, head_cols(k)] = res[k * 128:(k + 1) * 128]

    total = blocks * per_block
    for h in range(kv_heads):
        def body(i, _):
            attend(h, i // per_block, lax.rem(i, per_block))
            if h + 1 < kv_heads:
                guarded(i == 0, lambda: open_crossed(2 * h + 3))
                guarded(jnp.logical_and(i > 0, i < line), lambda: step(h + 1, i))
            return 0
        lax.fori_loop(0, total, body, 0)
        if h + 1 < kv_heads:
            for s in range(total, line):
                step(h + 1, s)
            finish(h + 1)

    quarter = o_ref.shape[1]
    parts = quarter // wide
    w_load.wait()

    def product(group, core, j):
        cols = pl.ds(pl.multiple_of((group * 2 + core) * quarter + j * wide, 128), wide)
        return jnp.dot(att[...], w[:, cols], preferred_element_type=jnp.float32)

    def pair_copy(i, j):
        return pltpu.make_async_remote_copy(
            src_ref=pair_out.at[i, j], dst_ref=pair_in.at[i, j], send_sem=pair_send.at[i, j],
            recv_sem=pair_recv.at[i, j], device_id=partner, device_id_type=MESH)

    def far_copy(i, j):
        return pltpu.make_async_remote_copy(
            src_ref=far_out.at[i, j], dst_ref=far_in.at[i, j], send_sem=far_send.at[i, j],
            recv_sem=far_recv.at[i, j], device_id=(me, far(i) * 2 + c), device_id_type=MESH)

    def far_step(k, _):
        i, j = 1 + k // parts, lax.rem(k, parts)
        pair_out[i, j] = product(far(i), 1 - c, j).astype(jnp.bfloat16)
        pair_copy(i, j).start()
        mine = product(far(i), c, j)
        pair_copy(i, j).wait_recv()
        far_out[i, j] = (mine + pair_in[i, j].astype(jnp.float32)).astype(jnp.bfloat16)
        far_copy(i, j).start()
        return 0
    lax.fori_loop(0, (groups - 1) * parts, far_step, 0)

    def near_step(j, _):
        pair_out[0, j] = product(y, 1 - c, j).astype(jnp.bfloat16)
        pair_copy(0, j).start()
        far_out[0, j] = product(y, c, j).astype(jnp.bfloat16)
        return 0
    lax.fori_loop(0, parts, near_step, 0)

    def close_step(j, _):
        pair_copy(0, j).wait_recv()
        res = far_out[0, j].astype(jnp.float32) + pair_in[0, j].astype(jnp.float32)
        for i in range(1, groups):
            far_copy(i, j).wait_recv()
            res = res + far_in[i, j].astype(jnp.float32)
        o_ref[:, pl.ds(pl.multiple_of(j * wide, 128), wide)] = res.astype(jnp.bfloat16)
        return 0
    lax.fori_loop(0, parts, close_step, 0)

    for d in range(1, n):
        order_copy(d, me, lax.rem(me + d, n)).wait_send()

    def drain(i, _):
        for p in range(2 * kv_heads):
            for side, tags in ((b, True), (other, p % 2 == 1)):
                blk = i * 2 + side
                if tags:
                    guarded(jnp.logical_and(a + 1 < line, i <= a),
                            lambda: piece(p, blk, 0, me + 2).wait_send())
                    guarded(jnp.logical_and(a > 0, i >= a),
                            lambda: piece(p, blk, 1, me - 2).wait_send())
            if p % 2 == 0:
                piece(p, i * 2 + b, 2, a * 2 + other).wait_send()
            else:
                guarded(i == a, lambda: piece(p, me, 2, a * 2 + other).wait_send())
        return 0
    lax.fori_loop(0, line, drain, 0)

    def drain_out(j, _):
        for i in range(groups):
            pair_copy(i, j).wait_send()
            if i:
                far_copy(i, j).wait_send()
        return 0
    lax.fori_loop(0, parts, drain_out, 0)


def shards(n, tp, queries, keys, values, out_weight, block_order):
    rows = queries.shape[0]
    heads = queries.shape[1] // HEAD_SIZE
    group = QUERY_HEADS // KEY_VALUE_HEADS
    kv_heads = max(1, heads // group)
    unit = min(2, heads // kv_heads)
    quarter = out_weight.shape[1] // tp
    wide = min(256, quarter)
    parts, groups, tokens, blocks = quarter // wide, tp // 2, n * rows, rows // 128
    dims = (n, tp, rows, heads, kv_heads, unit, wide)
    any_space = pl.BlockSpec(memory_space=pl.ANY)
    dma = pltpu.SemaphoreType.DMA
    bf16 = jnp.bfloat16
    swap = pltpu.VMEM((groups, parts, rows, wide), bf16)
    return pl.pallas_call(
        functools.partial(kernel, dims),
        out_shape=jax.ShapeDtypeStruct((rows, quarter), bf16),
        in_specs=[any_space] * 4 + [pl.BlockSpec(memory_space=pltpu.SMEM)],
        out_specs=pl.BlockSpec(memory_space=pltpu.VMEM),
        scratch_shapes=[
            pltpu.VMEM(queries.shape, bf16),
            pltpu.VMEM(out_weight.shape, bf16),
            pltpu.VMEM((2 * kv_heads, tokens, HEAD_SIZE), bf16),
            pltpu.VMEM((8, 128), jnp.int32),
            pltpu.VMEM((n, 8, 128), jnp.int32),
            pltpu.VMEM((blocks, tokens, 128), bf16),
            pltpu.VMEM((128, 128), bf16),
            pltpu.VMEM((unit * 128, tokens), jnp.float32),
            pltpu.VMEM((rows, heads * HEAD_SIZE), bf16),
            swap, swap, swap, swap,
            dma((2 * kv_heads + 2,)), dma((n,)), dma((n,)),
            dma((2 * kv_heads, n, 3)), dma((2 * kv_heads, n)),
            dma((groups, parts)), dma((groups, parts)), dma((groups, parts)), dma((groups, parts)),
        ],
        compiler_params=pltpu.CompilerParams(
            collective_id=0, has_side_effects=True, vmem_limit_bytes=60 * 2**20),
    )(queries, keys, values, out_weight, block_order)


def solution(mesh):
    n, tp = mesh.shape["ctx"], mesh.shape["tp"]
    in_specs = (P("ctx", "tp"), P("ctx", None), P("ctx", None), P("tp", None), P("ctx"))
    return jax.shard_map(functools.partial(shards, n, tp), mesh=mesh, in_specs=in_specs,
                         out_specs=P("ctx", "tp"), check_vma=False)
```

```python
import functools
import math

import jax
import jax.numpy as jnp
from jax import lax
from jax.experimental import pallas as pl
from jax.experimental.pallas import tpu as pltpu
from jax.sharding import PartitionSpec as P

QUERY_HEADS = 64
KEY_VALUE_HEADS = 8
HEAD_SIZE = 128
MESH = pl.DeviceIdType.MESH
NT = (((1,), (1,)), ((), ()))


def kernel(dims, q_hbm, k_hbm, v_hbm, w_hbm, order, o_ref, q, w, kv, tile, orders, mask, eye, scores,
           att, pair_out, pair_in, far_out, far_in, load_sem, order_send, order_recv, send, recv,
           pair_send, pair_recv, far_send, far_recv):
    n, tp, rows, heads, kv_heads, unit, wide = dims
    line, groups = n // 2, tp // 2
    tokens = n * rows
    blocks = rows // 128
    per_kv = heads // kv_heads
    me, t = lax.axis_index("ctx"), lax.axis_index("tp")
    a, b = me // 2, lax.rem(me, 2)
    y, c = t // 2, lax.rem(t, 2)
    other = 1 - b
    partner = (me, y * 2 + 1 - c)

    def far(i):
        return lax.rem(y + i, groups)

    first = t * heads // (QUERY_HEADS // KEY_VALUE_HEADS)
    own = pl.ds(pl.multiple_of(me * rows, 128), rows)
    loads = []
    for p in range(2 * kv_heads):
        src = v_hbm if p % 2 else k_hbm
        cols = pl.ds(pl.multiple_of((first + p // 2) * HEAD_SIZE, 128), HEAD_SIZE)
        loads.append(pltpu.make_async_copy(src.at[:, cols], kv.at[p, own, :], load_sem.at[p]))
        loads[-1].start()
    q_load = pltpu.make_async_copy(q_hbm, q, load_sem.at[2 * kv_heads])
    w_load = pltpu.make_async_copy(w_hbm, w, load_sem.at[2 * kv_heads + 1])
    q_load.start()
    w_load.start()
    for i in range(blocks):
        tile[pl.ds(i, 1), :] = jnp.full((1, 128), order[i], jnp.int32)

    barrier = pltpu.get_barrier_semaphore()
    for d in range(1, n):
        pl.semaphore_signal(barrier, inc=1, device_id=(lax.rem(me + d, n), t), device_id_type=MESH)
    pl.semaphore_signal(barrier, inc=1, device_id=partner, device_id_type=MESH)
    for i in range(1, groups):
        pl.semaphore_signal(barrier, inc=1, device_id=(me, far(i) * 2 + c), device_id_type=MESH)
    pl.semaphore_wait(barrier, n - 1 + 1 + groups - 1)

    def order_copy(d, src_dev, target):
        return pltpu.make_async_remote_copy(
            src_ref=tile, dst_ref=orders.at[src_dev], send_sem=order_send.at[d],
            recv_sem=order_recv.at[d], device_id=(target, t), device_id_type=MESH)

    def piece(p, block, way, target):
        at = pl.ds(pl.multiple_of(block * rows, 128), rows)
        return pltpu.make_async_remote_copy(
            src_ref=kv.at[p, at, :], dst_ref=kv.at[p, at, :], send_sem=send.at[p, block, way],
            recv_sem=recv.at[p, block], device_id=(target, t), device_id_type=MESH)

    def guarded(cond, act):
        pl.when(cond)(act)

    def open_line(p):
        guarded(a + 1 < line, lambda: piece(p, me, 0, me + 2).start())
        guarded(a > 0, lambda: piece(p, me, 1, me - 2).start())
        piece(p, me, 2, a * 2 + other).start()

    def open_crossed(p):
        blk = a * 2 + other
        piece(p, blk, 2, blk).wait_recv()
        guarded(a + 1 < line, lambda: piece(p, blk, 0, me + 2).start())
        guarded(a > 0, lambda: piece(p, blk, 1, me - 2).start())

    def relay(p, s, side, crossing):
        low, high = (a - s) * 2 + side, (a + s) * 2 + side

        @pl.when(a - s >= 0)
        def _():
            piece(p, low, 0, me).wait_recv()
            guarded(a + 1 < line, lambda: piece(p, low, 0, me + 2).start())
            if crossing:
                piece(p, low, 2, a * 2 + other).start()

        @pl.when(a + s < line)
        def _():
            piece(p, high, 1, me).wait_recv()
            guarded(a > 0, lambda: piece(p, high, 1, me - 2).start())
            if crossing:
                piece(p, high, 2, a * 2 + other).start()

    last = 2 * kv_heads - 1

    def step(h, s):
        for p in (2 * h, 2 * h + 1):
            relay(p, s, b, p != last)
            if p == last:
                relay(p, s, other, False)

    def finish(h):
        def body(i, _):
            for p in (2 * h, 2 * h + 1):
                if p != last:
                    piece(p, i * 2 + other, 2, me).wait_recv()
            return 0
        lax.fori_loop(0, line, body, 0)

    def open_own(p):
        loads[p].wait()
        open_line(p)

    for d in range(1, n):
        order_copy(d, me, lax.rem(me + d, n)).start()
    for p in range(max(2, last)):
        open_own(p)
    orders[pl.ds(me, 1)] = tile[...][None]
    row = lax.broadcasted_iota(jnp.int32, (128, 128), 0)
    col = lax.broadcasted_iota(jnp.int32, (128, 128), 1)
    eye[...] = (row == col).astype(jnp.bfloat16)
    if last == 1:
        open_crossed(1)
    step(0, 1)
    if last > 1:
        open_own(last)
    for d in range(1, n):
        order_copy(d, lax.rem(me + n - d, n), me).wait_recv()

    def build(i, _):
        for j in range(blocks):
            kpos = orders[pl.ds(i, 1), j:j + 1, :][0] * 128 + row
            for g in range(blocks):
                qpos = tile[g:g + 1, :] * 128 + col
                at = pl.ds(pl.multiple_of(i * rows + j * 128, 128), 128)
                mask[g, at, :] = jnp.where(kpos <= qpos, 0.0, -1e30).astype(jnp.bfloat16)
        return 0
    lax.fori_loop(0, n, build, 0)

    for s in range(2, line):
        step(0, s)
    finish(0)
    q_load.wait()

    chunk = tokens // 4
    factor = math.log2(math.e) / math.sqrt(HEAD_SIZE)
    ones = jnp.ones((chunk, 128), jnp.bfloat16)
    per_block = per_kv // unit

    def attend(h, g, u):
        at = pl.ds(pl.multiple_of(g * 128, 128), 128)
        def head_cols(k):
            return pl.ds(pl.multiple_of((h * per_kv + u * unit + k) * HEAD_SIZE, 128), HEAD_SIZE)
        e = eye[...]
        qa = jnp.concatenate(
            [jnp.concatenate([q[at, head_cols(k)], e], axis=1) for k in range(unit)], axis=0)
        top = None
        for i in range(4):
            ks = pl.ds(i * chunk, chunk)
            ka = jnp.concatenate([kv[2 * h, ks, :], mask[g, ks, :]], axis=1)
            s = lax.dot_general(qa, ka, NT, preferred_element_type=jnp.float32)
            scores[:, ks] = s
            for j in range(0, chunk, 128):
                part = s[:, j:j + 128]
                top = part if top is None else jnp.maximum(top, part)
        top = jnp.max(top, axis=1, keepdims=True)
        acc = None
        for i in range(4):
            ks = pl.ds(i * chunk, chunk)
            weight = jnp.exp2((scores[:, ks] - top) * factor).astype(jnp.bfloat16)
            va = jnp.concatenate([kv[2 * h + 1, ks, :], ones], axis=1)
            part = jnp.dot(weight, va, preferred_element_type=jnp.float32)
            acc = part if acc is None else acc + part
        res = (acc[:, :128] / acc[:, 128:]).astype(jnp.bfloat16)
        for k in range(unit):
            att[at, head_cols(k)] = res[k * 128:(k + 1) * 128]

    total = blocks * per_block
    for h in range(kv_heads):
        if h + 1 < kv_heads:
            if 2 * h + 3 == last:
                open_crossed(last)
            step(h + 1, 1)

        def body(i, _):
            attend(h, i // per_block, lax.rem(i, per_block))
            if h + 1 < kv_heads:
                s = (i + 3) // 2
                guarded(jnp.logical_and(lax.rem(i, 2) == 1, s < line), lambda: step(h + 1, s))
            return 0
        lax.fori_loop(0, total, body, 0)
        if h + 1 < kv_heads:
            for s in range(total // 2 + 2, line):
                step(h + 1, s)
            finish(h + 1)

    quarter = o_ref.shape[1]
    parts = quarter // wide
    w_load.wait()

    def product(group, core, j):
        cols = pl.ds(pl.multiple_of((group * 2 + core) * quarter + j * wide, 128), wide)
        return jnp.dot(att[...], w[:, cols], preferred_element_type=jnp.float32)

    def pair_copy(i, j):
        return pltpu.make_async_remote_copy(
            src_ref=pair_out.at[i, j], dst_ref=pair_in.at[i, j], send_sem=pair_send.at[i, j],
            recv_sem=pair_recv.at[i, j], device_id=partner, device_id_type=MESH)

    def far_copy(i, j):
        return pltpu.make_async_remote_copy(
            src_ref=far_out.at[i, j], dst_ref=far_in.at[i, j], send_sem=far_send.at[i, j],
            recv_sem=far_recv.at[i, j], device_id=(me, far(i) * 2 + c), device_id_type=MESH)

    def far_step(k, _):
        i, j = 1 + k // parts, lax.rem(k, parts)
        pair_out[i, j] = product(far(i), 1 - c, j).astype(jnp.bfloat16)
        pair_copy(i, j).start()
        mine = product(far(i), c, j)
        pair_copy(i, j).wait_recv()
        far_out[i, j] = (mine + pair_in[i, j].astype(jnp.float32)).astype(jnp.bfloat16)
        far_copy(i, j).start()
        return 0
    lax.fori_loop(0, (groups - 1) * parts, far_step, 0)

    def near_step(j, _):
        pair_out[0, j] = product(y, 1 - c, j).astype(jnp.bfloat16)
        pair_copy(0, j).start()
        far_out[0, j] = product(y, c, j).astype(jnp.bfloat16)
        return 0
    lax.fori_loop(0, parts, near_step, 0)

    def close_step(j, _):
        pair_copy(0, j).wait_recv()
        res = far_out[0, j].astype(jnp.float32) + pair_in[0, j].astype(jnp.float32)
        for i in range(1, groups):
            far_copy(i, j).wait_recv()
            res = res + far_in[i, j].astype(jnp.float32)
        o_ref[:, pl.ds(pl.multiple_of(j * wide, 128), wide)] = res.astype(jnp.bfloat16)
        return 0
    lax.fori_loop(0, parts, close_step, 0)

    for d in range(1, n):
        order_copy(d, me, lax.rem(me + d, n)).wait_send()

    def drain(i, _):
        for p in range(2 * kv_heads):
            for side, tags in ((b, True), (other, p == last)):
                blk = i * 2 + side
                if tags:
                    guarded(jnp.logical_and(a + 1 < line, i <= a),
                            lambda: piece(p, blk, 0, me + 2).wait_send())
                    guarded(jnp.logical_and(a > 0, i >= a),
                            lambda: piece(p, blk, 1, me - 2).wait_send())
            if p != last:
                piece(p, i * 2 + b, 2, a * 2 + other).wait_send()
            else:
                guarded(i == a, lambda: piece(p, me, 2, a * 2 + other).wait_send())
        return 0
    lax.fori_loop(0, line, drain, 0)

    def drain_out(j, _):
        for i in range(groups):
            pair_copy(i, j).wait_send()
            if i:
                far_copy(i, j).wait_send()
        return 0
    lax.fori_loop(0, parts, drain_out, 0)


def shards(n, tp, queries, keys, values, out_weight, block_order):
    rows = queries.shape[0]
    heads = queries.shape[1] // HEAD_SIZE
    group = QUERY_HEADS // KEY_VALUE_HEADS
    kv_heads = max(1, heads // group)
    unit = min(2, heads // kv_heads)
    quarter = out_weight.shape[1] // tp
    wide = min(256, quarter)
    parts, groups, tokens, blocks = quarter // wide, tp // 2, n * rows, rows // 128
    dims = (n, tp, rows, heads, kv_heads, unit, wide)
    any_space = pl.BlockSpec(memory_space=pl.ANY)
    dma = pltpu.SemaphoreType.DMA
    bf16 = jnp.bfloat16
    swap = pltpu.VMEM((groups, parts, rows, wide), bf16)
    return pl.pallas_call(
        functools.partial(kernel, dims),
        out_shape=jax.ShapeDtypeStruct((rows, quarter), bf16),
        in_specs=[any_space] * 4 + [pl.BlockSpec(memory_space=pltpu.SMEM)],
        out_specs=pl.BlockSpec(memory_space=pltpu.VMEM),
        scratch_shapes=[
            pltpu.VMEM(queries.shape, bf16),
            pltpu.VMEM(out_weight.shape, bf16),
            pltpu.VMEM((2 * kv_heads, tokens, HEAD_SIZE), bf16),
            pltpu.VMEM((8, 128), jnp.int32),
            pltpu.VMEM((n, 8, 128), jnp.int32),
            pltpu.VMEM((blocks, tokens, 128), bf16),
            pltpu.VMEM((128, 128), bf16),
            pltpu.VMEM((unit * 128, tokens), jnp.float32),
            pltpu.VMEM((rows, heads * HEAD_SIZE), bf16),
            swap, swap, swap, swap,
            dma((2 * kv_heads + 2,)), dma((n,)), dma((n,)),
            dma((2 * kv_heads, n, 3)), dma((2 * kv_heads, n)),
            dma((groups, parts)), dma((groups, parts)), dma((groups, parts)), dma((groups, parts)),
        ],
        compiler_params=pltpu.CompilerParams(
            collective_id=0, has_side_effects=True, vmem_limit_bytes=60 * 2**20),
    )(queries, keys, values, out_weight, block_order)


def solution(mesh):
    n, tp = mesh.shape["ctx"], mesh.shape["tp"]
    in_specs = (P("ctx", "tp"), P("ctx", None), P("ctx", None), P("tp", None), P("ctx"))
    return jax.shard_map(functools.partial(shards, n, tp), mesh=mesh, in_specs=in_specs,
                         out_specs=P("ctx", "tp"), check_vma=False)
```

```python
import functools
import math

import jax
import jax.numpy as jnp
from jax import lax
from jax.experimental import pallas as pl
from jax.experimental.pallas import tpu as pltpu
from jax.sharding import PartitionSpec as P

QUERY_HEADS = 64
KEY_VALUE_HEADS = 8
HEAD_SIZE = 128
MESH = pl.DeviceIdType.MESH
NT = (((1,), (1,)), ((), ()))


def kernel(dims, q_hbm, k_hbm, v_hbm, w_hbm, order, o_ref, q, w, kv, orders, mask, eye, scores,
           att, pair_out, pair_in, far_out, far_in, load_sem, send, recv,
           pair_send, pair_recv, far_send, far_recv):
    n, tp, rows, heads, kv_heads, unit, wide = dims
    line, groups = n // 2, tp // 2
    tokens = n * rows
    blocks = rows // 128
    per_kv = heads // kv_heads
    me, t = lax.axis_index("ctx"), lax.axis_index("tp")
    a, b = me // 2, lax.rem(me, 2)
    y, c = t // 2, lax.rem(t, 2)
    other = 1 - b
    partner = (me, y * 2 + 1 - c)

    def far(i):
        return lax.rem(y + i, groups)

    first = t * heads // (QUERY_HEADS // KEY_VALUE_HEADS)
    own = pl.ds(pl.multiple_of(me * rows, 128), rows)
    loads = []
    for p in range(2 * kv_heads):
        src = v_hbm if p % 2 else k_hbm
        cols = pl.ds(pl.multiple_of((first + p // 2) * HEAD_SIZE, 128), HEAD_SIZE)
        loads.append(pltpu.make_async_copy(src.at[:, cols], kv.at[p, own, :], load_sem.at[p]))
        loads[-1].start()
    q_load = pltpu.make_async_copy(q_hbm, q, load_sem.at[2 * kv_heads])
    w_load = pltpu.make_async_copy(w_hbm, w, load_sem.at[2 * kv_heads + 1])
    q_load.start()
    w_load.start()
    for i in range(blocks):
        orders[pl.ds(me, 1), i:i + 1, :] = jnp.full((1, 1, 128), order[i], jnp.int32)

    def guarded(cond, act):
        pl.when(cond)(act)

    up, down, across = a + 1 < line, a > 0, a * 2 + other

    barrier = pltpu.get_barrier_semaphore()

    def greet(target):
        pl.semaphore_signal(barrier, inc=1, device_id=target, device_id_type=MESH)

    guarded(up, lambda: greet((me + 2, t)))
    guarded(down, lambda: greet((me - 2, t)))
    greet((across, t))
    greet(partner)
    for i in range(1, groups):
        greet((me, far(i) * 2 + c))
    pl.semaphore_wait(barrier, 1 + groups + up.astype(jnp.int32) + down.astype(jnp.int32))

    marks = 2 * kv_heads

    def piece(p, block, way, target):
        at = pl.ds(pl.multiple_of(block * rows, 128), rows)
        ref = orders.at[block] if p == marks else kv.at[p, at, :]
        return pltpu.make_async_remote_copy(
            src_ref=ref, dst_ref=ref, send_sem=send.at[p, block, way],
            recv_sem=recv.at[p, block], device_id=(target, t), device_id_type=MESH)

    def open_own(p):
        if p != marks:
            loads[p].wait()
        guarded(up, lambda: piece(p, me, 0, me + 2).start())
        guarded(down, lambda: piece(p, me, 1, me - 2).start())
        piece(p, me, 2, across).start()

    def relay(p, s):
        low, high = me - 2 * s, me + 2 * s

        @pl.when(a - s >= 0)
        def _():
            piece(p, low, 0, me).wait_recv()
            guarded(up, lambda: piece(p, low, 0, me + 2).start())
            piece(p, low, 2, across).start()

        @pl.when(a + s < line)
        def _():
            piece(p, high, 1, me).wait_recv()
            guarded(down, lambda: piece(p, high, 1, me - 2).start())
            piece(p, high, 2, across).start()

    def step(h, s):
        for p in (2 * h, 2 * h + 1):
            relay(p, s)

    def finish(h):
        def body(i, _):
            for p in (2 * h, 2 * h + 1):
                piece(p, i * 2 + other, 2, me).wait_recv()
            return 0
        lax.fori_loop(0, line, body, 0)

    row = lax.broadcasted_iota(jnp.int32, (128, 128), 0)
    col = lax.broadcasted_iota(jnp.int32, (128, 128), 1)

    def build(i):
        for j in range(blocks):
            kpos = orders[pl.ds(i, 1), j:j + 1, :][0] * 128 + row
            for g in range(blocks):
                qpos = orders[pl.ds(me, 1), g:g + 1, :][0] * 128 + col
                at = pl.ds(pl.multiple_of(i * rows + j * 128, 128), 128)
                mask[g, at, :] = jnp.where(kpos <= qpos, 0.0, -1e30).astype(jnp.bfloat16)

    def build_crossed(s):
        def one(i):
            piece(marks, i, 2, me).wait_recv()
            build(i)
        guarded(a - s >= 0, lambda: one(across - 2 * s))
        guarded(jnp.logical_and(s > 0, a + s < line), lambda: one(across + 2 * s))

    open_own(marks)
    early = min(3, 2 * kv_heads)
    for p in range(early):
        open_own(p)
    eye[...] = (row == col).astype(jnp.bfloat16)
    build(me)

    def first_head(s, _):
        relay(marks, s)
        step(0, s)
        if kv_heads > 1:
            @pl.when(s == 1)
            def _():
                for p in range(early, 2 * kv_heads):
                    open_own(p)
            guarded(s > 1, lambda: step(1, s - 1))
        guarded(a - s >= 0, lambda: build(me - 2 * s))
        guarded(a + s < line, lambda: build(me + 2 * s))
        build_crossed(s - 1)
        return 0
    lax.fori_loop(1, line, first_head, 0)
    build_crossed(jnp.int32(line - 1))
    finish(0)
    q_load.wait()

    chunk = tokens // 4
    factor = math.log2(math.e) / math.sqrt(HEAD_SIZE)
    ones = jnp.ones((chunk, 128), jnp.bfloat16)
    per_block = per_kv // unit

    def attend(h, g, u):
        at = pl.ds(pl.multiple_of(g * 128, 128), 128)
        def head_cols(k):
            return pl.ds(pl.multiple_of((h * per_kv + u * unit + k) * HEAD_SIZE, 128), HEAD_SIZE)
        e = eye[...]
        qa = jnp.concatenate(
            [jnp.concatenate([q[at, head_cols(k)], e], axis=1) for k in range(unit)], axis=0)
        top = None
        for i in range(4):
            ks = pl.ds(i * chunk, chunk)
            ka = jnp.concatenate([kv[2 * h, ks, :], mask[g, ks, :]], axis=1)
            s = lax.dot_general(qa, ka, NT, preferred_element_type=jnp.float32)
            scores[:, ks] = s
            for j in range(0, chunk, 128):
                part = s[:, j:j + 128]
                top = part if top is None else jnp.maximum(top, part)
        top = jnp.max(top, axis=1, keepdims=True)
        acc = None
        for i in range(4):
            ks = pl.ds(i * chunk, chunk)
            weight = jnp.exp2((scores[:, ks] - top) * factor).astype(jnp.bfloat16)
            va = jnp.concatenate([kv[2 * h + 1, ks, :], ones], axis=1)
            part = jnp.dot(weight, va, preferred_element_type=jnp.float32)
            acc = part if acc is None else acc + part
        res = (acc[:, :128] / acc[:, 128:]).astype(jnp.bfloat16)
        for k in range(unit):
            att[at, head_cols(k)] = res[k * 128:(k + 1) * 128]

    total = blocks * per_block
    for h in range(kv_heads):
        def body(i, _):
            attend(h, i // per_block, lax.rem(i, per_block))
            if h == 0 and kv_heads > 1:
                guarded(i == 1, lambda: step(1, line - 1))
            return 0
        lax.fori_loop(0, total, body, 0)
        if h + 1 < kv_heads:
            for s in range(1 if h else line - 1, line) if (h or total < 2) else ():
                step(h + 1, s)
            finish(h + 1)

    quarter = o_ref.shape[1]
    parts = quarter // wide
    w_load.wait()

    def product(group, core, j):
        cols = pl.ds(pl.multiple_of((group * 2 + core) * quarter + j * wide, 128), wide)
        return jnp.dot(att[...], w[:, cols], preferred_element_type=jnp.float32)

    def pair_copy(i, j):
        return pltpu.make_async_remote_copy(
            src_ref=pair_out.at[i, j], dst_ref=pair_in.at[i, j], send_sem=pair_send.at[i, j],
            recv_sem=pair_recv.at[i, j], device_id=partner, device_id_type=MESH)

    def far_copy(i, j):
        return pltpu.make_async_remote_copy(
            src_ref=far_out.at[i, j], dst_ref=far_in.at[i, j], send_sem=far_send.at[i, j],
            recv_sem=far_recv.at[i, j], device_id=(me, far(i) * 2 + c), device_id_type=MESH)

    def far_step(k, _):
        i, j = 1 + k // parts, lax.rem(k, parts)
        pair_out[i, j] = product(far(i), 1 - c, j).astype(jnp.bfloat16)
        pair_copy(i, j).start()
        mine = product(far(i), c, j)
        pair_copy(i, j).wait_recv()
        far_out[i, j] = (mine + pair_in[i, j].astype(jnp.float32)).astype(jnp.bfloat16)
        far_copy(i, j).start()
        return 0
    lax.fori_loop(0, (groups - 1) * parts, far_step, 0)

    def near_step(j, _):
        pair_out[0, j] = product(y, 1 - c, j).astype(jnp.bfloat16)
        pair_copy(0, j).start()
        far_out[0, j] = product(y, c, j).astype(jnp.bfloat16)
        return 0
    lax.fori_loop(0, parts, near_step, 0)

    def close_step(j, _):
        pair_copy(0, j).wait_recv()
        res = far_out[0, j].astype(jnp.float32) + pair_in[0, j].astype(jnp.float32)
        for i in range(1, groups):
            far_copy(i, j).wait_recv()
            res = res + far_in[i, j].astype(jnp.float32)
        o_ref[:, pl.ds(pl.multiple_of(j * wide, 128), wide)] = res.astype(jnp.bfloat16)
        return 0
    lax.fori_loop(0, parts, close_step, 0)

    def drain(i, _):
        for p in range(2 * kv_heads + 1):
            blk = i * 2 + b
            guarded(jnp.logical_and(up, i <= a), lambda: piece(p, blk, 0, me + 2).wait_send())
            guarded(jnp.logical_and(down, i >= a), lambda: piece(p, blk, 1, me - 2).wait_send())
            piece(p, blk, 2, across).wait_send()
        return 0
    lax.fori_loop(0, line, drain, 0)

    def drain_out(j, _):
        for i in range(groups):
            pair_copy(i, j).wait_send()
            if i:
                far_copy(i, j).wait_send()
        return 0
    lax.fori_loop(0, parts, drain_out, 0)


def shards(n, tp, queries, keys, values, out_weight, block_order):
    rows = queries.shape[0]
    heads = queries.shape[1] // HEAD_SIZE
    group = QUERY_HEADS // KEY_VALUE_HEADS
    kv_heads = max(1, heads // group)
    unit = min(2, heads // kv_heads)
    quarter = out_weight.shape[1] // tp
    wide = min(256, quarter)
    parts, groups, tokens, blocks = quarter // wide, tp // 2, n * rows, rows // 128
    dims = (n, tp, rows, heads, kv_heads, unit, wide)
    any_space = pl.BlockSpec(memory_space=pl.ANY)
    dma = pltpu.SemaphoreType.DMA
    bf16 = jnp.bfloat16
    swap = pltpu.VMEM((groups, parts, rows, wide), bf16)
    return pl.pallas_call(
        functools.partial(kernel, dims),
        out_shape=jax.ShapeDtypeStruct((rows, quarter), bf16),
        in_specs=[any_space] * 4 + [pl.BlockSpec(memory_space=pltpu.SMEM)],
        out_specs=pl.BlockSpec(memory_space=pltpu.VMEM),
        scratch_shapes=[
            pltpu.VMEM(queries.shape, bf16),
            pltpu.VMEM(out_weight.shape, bf16),
            pltpu.VMEM((2 * kv_heads, tokens, HEAD_SIZE), bf16),
            pltpu.VMEM((n, 8, 128), jnp.int32),
            pltpu.VMEM((blocks, tokens, 128), bf16),
            pltpu.VMEM((128, 128), bf16),
            pltpu.VMEM((unit * 128, tokens), jnp.float32),
            pltpu.VMEM((rows, heads * HEAD_SIZE), bf16),
            swap, swap, swap, swap,
            dma((2 * kv_heads + 2,)),
            dma((2 * kv_heads + 1, n, 3)), dma((2 * kv_heads + 1, n)),
            dma((groups, parts)), dma((groups, parts)), dma((groups, parts)), dma((groups, parts)),
        ],
        compiler_params=pltpu.CompilerParams(
            collective_id=0, has_side_effects=True, vmem_limit_bytes=60 * 2**20),
    )(queries, keys, values, out_weight, block_order)


def solution(mesh):
    n, tp = mesh.shape["ctx"], mesh.shape["tp"]
    in_specs = (P("ctx", "tp"), P("ctx", None), P("ctx", None), P("tp", None), P("ctx"))
    return jax.shard_map(functools.partial(shards, n, tp), mesh=mesh, in_specs=in_specs,
                         out_specs=P("ctx", "tp"), check_vma=False)
```

```python
import functools
import math

import jax
import jax.numpy as jnp
from jax import lax
from jax.experimental import pallas as pl
from jax.experimental.pallas import tpu as pltpu
from jax.sharding import PartitionSpec as P

QUERY_HEADS = 64
KEY_VALUE_HEADS = 8
HEAD_SIZE = 128
MESH = pl.DeviceIdType.MESH
NT = (((1,), (1,)), ((), ()))


def kernel(dims, q_hbm, k_hbm, v_hbm, w_hbm, order, o_ref, q, w, kv, orders, mask, eye, scores,
           att, pair_out, pair_in, far_out, far_in, load_sem, send, recv,
           pair_send, pair_recv, far_send, far_recv):
    n, tp, rows, heads, kv_heads, unit, wide = dims
    line, groups = n // 2, tp // 2
    tokens = n * rows
    blocks = rows // 128
    per_kv = heads // kv_heads
    me, t = lax.axis_index("ctx"), lax.axis_index("tp")
    a, b = me // 2, lax.rem(me, 2)
    y, c = t // 2, lax.rem(t, 2)
    other = 1 - b
    partner = (me, y * 2 + 1 - c)

    def far(i):
        return lax.rem(y + i, groups)

    first = t * heads // (QUERY_HEADS // KEY_VALUE_HEADS)
    own = pl.ds(pl.multiple_of(me * rows, 128), rows)
    loads = []
    for p in range(2 * kv_heads):
        src = v_hbm if p % 2 else k_hbm
        cols = pl.ds(pl.multiple_of((first + p // 2) * HEAD_SIZE, 128), HEAD_SIZE)
        loads.append(pltpu.make_async_copy(src.at[:, cols], kv.at[p, own, :], load_sem.at[p]))
        loads[-1].start()
    q_load = pltpu.make_async_copy(q_hbm, q, load_sem.at[2 * kv_heads])
    w_load = pltpu.make_async_copy(w_hbm, w, load_sem.at[2 * kv_heads + 1])
    q_load.start()
    w_load.start()
    for i in range(blocks):
        orders[pl.ds(me, 1), i:i + 1, :] = jnp.full((1, 1, 128), order[i], jnp.int32)

    def guarded(cond, act):
        pl.when(cond)(act)

    up, down, across = a + 1 < line, a > 0, a * 2 + other

    barrier = pltpu.get_barrier_semaphore()

    def greet(target):
        pl.semaphore_signal(barrier, inc=1, device_id=target, device_id_type=MESH)

    guarded(up, lambda: greet((me + 2, t)))
    guarded(down, lambda: greet((me - 2, t)))
    greet((across, t))
    greet(partner)
    for i in range(1, groups):
        greet((me, far(i) * 2 + c))
    pl.semaphore_wait(barrier, 1 + groups + up.astype(jnp.int32) + down.astype(jnp.int32))

    marks = 2 * kv_heads

    def piece(p, block, way, target):
        at = pl.ds(pl.multiple_of(block * rows, 128), rows)
        ref = orders.at[block] if p == marks else kv.at[p, at, :]
        return pltpu.make_async_remote_copy(
            src_ref=ref, dst_ref=ref, send_sem=send.at[p, block, way],
            recv_sem=recv.at[p, block], device_id=(target, t), device_id_type=MESH)

    def open_own(p, crossing=True):
        if p != marks:
            loads[p].wait()
        guarded(up, lambda: piece(p, me, 0, me + 2).start())
        guarded(down, lambda: piece(p, me, 1, me - 2).start())
        if crossing:
            piece(p, me, 2, across).start()

    def relay(p, s, crossing=True):
        low, high = me - 2 * s, me + 2 * s

        @pl.when(a - s >= 0)
        def _():
            piece(p, low, 0, me).wait_recv()
            guarded(up, lambda: piece(p, low, 0, me + 2).start())
            if crossing:
                piece(p, low, 2, across).start()

        @pl.when(a + s < line)
        def _():
            piece(p, high, 1, me).wait_recv()
            guarded(down, lambda: piece(p, high, 1, me - 2).start())
            if crossing:
                piece(p, high, 2, across).start()

    def step(h, s, crossing=True):
        for p in (2 * h, 2 * h + 1):
            relay(p, s, crossing)

    def cross_held(h):
        for p in (2 * h, 2 * h + 1):
            piece(p, me, 2, across).start()
        for s in range(1, line - 1):
            for p in (2 * h, 2 * h + 1):
                guarded(a - s >= 0, lambda: piece(p, me - 2 * s, 2, across).start())
                guarded(a + s < line, lambda: piece(p, me + 2 * s, 2, across).start())

    def finish(h):
        def body(i, _):
            for p in (2 * h, 2 * h + 1):
                piece(p, i * 2 + other, 2, me).wait_recv()
            return 0
        lax.fori_loop(0, line, body, 0)

    row = lax.broadcasted_iota(jnp.int32, (128, 128), 0)
    col = lax.broadcasted_iota(jnp.int32, (128, 128), 1)

    def build(i):
        for j in range(blocks):
            kpos = orders[pl.ds(i, 1), j:j + 1, :][0] * 128 + row
            for g in range(blocks):
                qpos = orders[pl.ds(me, 1), g:g + 1, :][0] * 128 + col
                at = pl.ds(pl.multiple_of(i * rows + j * 128, 128), 128)
                mask[g, at, :] = jnp.where(kpos <= qpos, 0.0, -1e30).astype(jnp.bfloat16)

    def build_crossed(s):
        def one(i):
            piece(marks, i, 2, me).wait_recv()
            build(i)
        guarded(a - s >= 0, lambda: one(across - 2 * s))
        guarded(jnp.logical_and(s > 0, a + s < line), lambda: one(across + 2 * s))

    open_own(marks)
    early = 2 if line > 2 else 2 * kv_heads
    for p in range(early):
        open_own(p, p // 2 != 1)
    eye[...] = (row == col).astype(jnp.bfloat16)
    build(me)

    def first_head(s, _):
        relay(marks, s)
        step(0, s)
        if kv_heads > 1:
            for p in range(early, 2 * kv_heads):
                guarded(s == min(p - 1, 2), lambda p=p: open_own(p, p // 2 != 1))
        guarded(a - s >= 0, lambda: build(me - 2 * s))
        guarded(a + s < line, lambda: build(me + 2 * s))
        build_crossed(s - 1)
        return 0
    lax.fori_loop(1, line, first_head, 0)
    if kv_heads > 1 and line > 2:
        step(1, 1, False)
    build_crossed(jnp.int32(line - 1))
    finish(0)
    if kv_heads > 1:
        for s in range(2, line - 1):
            step(1, s, False)
        cross_held(1)
    q_load.wait()

    chunk = tokens // 4
    factor = math.log2(math.e) / math.sqrt(HEAD_SIZE)
    ones = jnp.ones((chunk, 128), jnp.bfloat16)
    per_block = per_kv // unit

    def attend(h, g, u):
        at = pl.ds(pl.multiple_of(g * 128, 128), 128)
        def head_cols(k):
            return pl.ds(pl.multiple_of((h * per_kv + u * unit + k) * HEAD_SIZE, 128), HEAD_SIZE)
        e = eye[...]
        qa = jnp.concatenate(
            [jnp.concatenate([q[at, head_cols(k)], e], axis=1) for k in range(unit)], axis=0)
        top = None
        for i in range(4):
            ks = pl.ds(i * chunk, chunk)
            ka = jnp.concatenate([kv[2 * h, ks, :], mask[g, ks, :]], axis=1)
            s = lax.dot_general(qa, ka, NT, preferred_element_type=jnp.float32)
            scores[:, ks] = s
            for j in range(0, chunk, 128):
                part = s[:, j:j + 128]
                top = part if top is None else jnp.maximum(top, part)
        top = jnp.max(top, axis=1, keepdims=True)
        acc = None
        for i in range(4):
            ks = pl.ds(i * chunk, chunk)
            weight = jnp.exp2((scores[:, ks] - top) * factor).astype(jnp.bfloat16)
            va = jnp.concatenate([kv[2 * h + 1, ks, :], ones], axis=1)
            part = jnp.dot(weight, va, preferred_element_type=jnp.float32)
            acc = part if acc is None else acc + part
        res = (acc[:, :128] / acc[:, 128:]).astype(jnp.bfloat16)
        for k in range(unit):
            att[at, head_cols(k)] = res[k * 128:(k + 1) * 128]

    total = blocks * per_block
    for h in range(kv_heads):
        def body(i, _):
            attend(h, i // per_block, lax.rem(i, per_block))
            if h == 0 and kv_heads > 1:
                guarded(i == 0, lambda: step(1, line - 1))
            return 0
        lax.fori_loop(0, total, body, 0)
        if h + 1 < kv_heads:
            for s in range(1 if h else line - 1, line) if (h or total < 2) else ():
                step(h + 1, s)
            finish(h + 1)

    quarter = o_ref.shape[1]
    parts = quarter // wide
    w_load.wait()

    def product(group, core, j):
        cols = pl.ds(pl.multiple_of((group * 2 + core) * quarter + j * wide, 128), wide)
        return jnp.dot(att[...], w[:, cols], preferred_element_type=jnp.float32)

    def pair_copy(i, j):
        return pltpu.make_async_remote_copy(
            src_ref=pair_out.at[i, j], dst_ref=pair_in.at[i, j], send_sem=pair_send.at[i, j],
            recv_sem=pair_recv.at[i, j], device_id=partner, device_id_type=MESH)

    def far_copy(i, j):
        return pltpu.make_async_remote_copy(
            src_ref=far_out.at[i, j], dst_ref=far_in.at[i, j], send_sem=far_send.at[i, j],
            recv_sem=far_recv.at[i, j], device_id=(me, far(i) * 2 + c), device_id_type=MESH)

    def far_step(k, _):
        i, j = 1 + k // parts, lax.rem(k, parts)
        pair_out[i, j] = product(far(i), 1 - c, j).astype(jnp.bfloat16)
        pair_copy(i, j).start()
        mine = product(far(i), c, j)
        pair_copy(i, j).wait_recv()
        far_out[i, j] = (mine + pair_in[i, j].astype(jnp.float32)).astype(jnp.bfloat16)
        far_copy(i, j).start()
        return 0
    lax.fori_loop(0, (groups - 1) * parts, far_step, 0)

    def near_step(j, _):
        pair_out[0, j] = product(y, 1 - c, j).astype(jnp.bfloat16)
        pair_copy(0, j).start()
        far_out[0, j] = product(y, c, j).astype(jnp.bfloat16)
        return 0
    lax.fori_loop(0, parts, near_step, 0)

    def close_step(j, _):
        pair_copy(0, j).wait_recv()
        res = far_out[0, j].astype(jnp.float32) + pair_in[0, j].astype(jnp.float32)
        for i in range(1, groups):
            far_copy(i, j).wait_recv()
            res = res + far_in[i, j].astype(jnp.float32)
        o_ref[:, pl.ds(pl.multiple_of(j * wide, 128), wide)] = res.astype(jnp.bfloat16)
        return 0
    lax.fori_loop(0, parts, close_step, 0)

    def drain(i, _):
        for p in range(2 * kv_heads + 1):
            blk = i * 2 + b
            guarded(jnp.logical_and(up, i <= a), lambda: piece(p, blk, 0, me + 2).wait_send())
            guarded(jnp.logical_and(down, i >= a), lambda: piece(p, blk, 1, me - 2).wait_send())
            piece(p, blk, 2, across).wait_send()
        return 0
    lax.fori_loop(0, line, drain, 0)

    def drain_out(j, _):
        for i in range(groups):
            pair_copy(i, j).wait_send()
            if i:
                far_copy(i, j).wait_send()
        return 0
    lax.fori_loop(0, parts, drain_out, 0)


def shards(n, tp, queries, keys, values, out_weight, block_order):
    rows = queries.shape[0]
    heads = queries.shape[1] // HEAD_SIZE
    group = QUERY_HEADS // KEY_VALUE_HEADS
    kv_heads = max(1, heads // group)
    unit = min(4, heads // kv_heads)
    quarter = out_weight.shape[1] // tp
    wide = min(256, quarter)
    parts, groups, tokens, blocks = quarter // wide, tp // 2, n * rows, rows // 128
    dims = (n, tp, rows, heads, kv_heads, unit, wide)
    any_space = pl.BlockSpec(memory_space=pl.ANY)
    dma = pltpu.SemaphoreType.DMA
    bf16 = jnp.bfloat16
    swap = pltpu.VMEM((groups, parts, rows, wide), bf16)
    return pl.pallas_call(
        functools.partial(kernel, dims),
        out_shape=jax.ShapeDtypeStruct((rows, quarter), bf16),
        in_specs=[any_space] * 4 + [pl.BlockSpec(memory_space=pltpu.SMEM)],
        out_specs=pl.BlockSpec(memory_space=pltpu.VMEM),
        scratch_shapes=[
            pltpu.VMEM(queries.shape, bf16),
            pltpu.VMEM(out_weight.shape, bf16),
            pltpu.VMEM((2 * kv_heads, tokens, HEAD_SIZE), bf16),
            pltpu.VMEM((n, 8, 128), jnp.int32),
            pltpu.VMEM((blocks, tokens, 128), bf16),
            pltpu.VMEM((128, 128), bf16),
            pltpu.VMEM((unit * 128, tokens), jnp.float32),
            pltpu.VMEM((rows, heads * HEAD_SIZE), bf16),
            swap, swap, swap, swap,
            dma((2 * kv_heads + 2,)),
            dma((2 * kv_heads + 1, n, 3)), dma((2 * kv_heads + 1, n)),
            dma((groups, parts)), dma((groups, parts)), dma((groups, parts)), dma((groups, parts)),
        ],
        compiler_params=pltpu.CompilerParams(
            collective_id=0, has_side_effects=True, vmem_limit_bytes=60 * 2**20),
    )(queries, keys, values, out_weight, block_order)


def solution(mesh):
    n, tp = mesh.shape["ctx"], mesh.shape["tp"]
    in_specs = (P("ctx", "tp"), P("ctx", None), P("ctx", None), P("tp", None), P("ctx"))
    return jax.shard_map(functools.partial(shards, n, tp), mesh=mesh, in_specs=in_specs,
                         out_specs=P("ctx", "tp"), check_vma=False)
```

```python
import functools
import math

import jax
import jax.numpy as jnp
from jax import lax
from jax.experimental import pallas as pl
from jax.experimental.pallas import tpu as pltpu
from jax.sharding import PartitionSpec as P

QUERY_HEADS = 64
KEY_VALUE_HEADS = 8
HEAD_SIZE = 128
MESH = pl.DeviceIdType.MESH
NT = (((1,), (1,)), ((), ()))


def kernel(dims, q_hbm, k_hbm, v_hbm, w_hbm, order, o_ref, q, w, kv, orders, mask, eye, scores,
           att, pair_out, pair_in, far_out, far_in, load_sem, send, recv,
           pair_send, pair_recv, far_send, far_recv):
    n, tp, rows, heads, kv_heads, unit, wide = dims
    line, groups = n // 2, tp // 2
    tokens = n * rows
    blocks = rows // 128
    per_kv = heads // kv_heads
    me, t = lax.axis_index("ctx"), lax.axis_index("tp")
    a, b = me // 2, lax.rem(me, 2)
    y, c = t // 2, lax.rem(t, 2)
    other = 1 - b
    partner = (me, y * 2 + 1 - c)

    def far(i):
        return lax.rem(y + i, groups)

    first = t * heads // (QUERY_HEADS // KEY_VALUE_HEADS)
    own = pl.ds(pl.multiple_of(me * rows, 128), rows)
    loads = []
    for p in range(2 * kv_heads):
        src = v_hbm if p % 2 else k_hbm
        cols = pl.ds(pl.multiple_of((first + p // 2) * HEAD_SIZE, 128), HEAD_SIZE)
        loads.append(pltpu.make_async_copy(src.at[:, cols], kv.at[p, own, :], load_sem.at[p]))
        loads[-1].start()
    q_load = pltpu.make_async_copy(q_hbm, q, load_sem.at[2 * kv_heads])
    w_load = pltpu.make_async_copy(w_hbm, w, load_sem.at[2 * kv_heads + 1])
    q_load.start()
    w_load.start()
    for i in range(blocks):
        orders[pl.ds(me, 1), i:i + 1, :] = jnp.full((1, 1, 128), order[i], jnp.int32)

    def guarded(cond, act):
        pl.when(cond)(act)

    up, down, across = a + 1 < line, a > 0, a * 2 + other

    barrier = pltpu.get_barrier_semaphore()

    def greet(target):
        pl.semaphore_signal(barrier, inc=1, device_id=target, device_id_type=MESH)

    guarded(up, lambda: greet((me + 2, t)))
    guarded(down, lambda: greet((me - 2, t)))
    greet((across, t))
    greet(partner)
    for i in range(1, groups):
        greet((me, far(i) * 2 + c))
    pl.semaphore_wait(barrier, 1 + groups + up.astype(jnp.int32) + down.astype(jnp.int32))

    marks = 2 * kv_heads

    def piece(p, block, way, target):
        at = pl.ds(pl.multiple_of(block * rows, 128), rows)
        ref = orders.at[block] if p == marks else kv.at[p, at, :]
        return pltpu.make_async_remote_copy(
            src_ref=ref, dst_ref=ref, send_sem=send.at[p, block, way],
            recv_sem=recv.at[p, block], device_id=(target, t), device_id_type=MESH)

    def open_own(p):
        if p != marks:
            loads[p].wait()
        guarded(up, lambda: piece(p, me, 0, me + 2).start())
        guarded(down, lambda: piece(p, me, 1, me - 2).start())
        piece(p, me, 2, across).start()

    def relay(p, s):
        low, high = me - 2 * s, me + 2 * s

        @pl.when(a - s >= 0)
        def _():
            piece(p, low, 0, me).wait_recv()
            guarded(up, lambda: piece(p, low, 0, me + 2).start())
            piece(p, low, 2, across).start()

        @pl.when(a + s < line)
        def _():
            piece(p, high, 1, me).wait_recv()
            guarded(down, lambda: piece(p, high, 1, me - 2).start())
            piece(p, high, 2, across).start()

    def step(h, s):
        for p in (2 * h, 2 * h + 1):
            relay(p, s)

    def finish(h):
        def body(i, _):
            for p in (2 * h, 2 * h + 1):
                piece(p, i * 2 + other, 2, me).wait_recv()
            return 0
        lax.fori_loop(0, line, body, 0)

    row = lax.broadcasted_iota(jnp.int32, (128, 128), 0)
    col = lax.broadcasted_iota(jnp.int32, (128, 128), 1)

    def build(i):
        for j in range(blocks):
            kpos = orders[pl.ds(i, 1), j:j + 1, :][0] * 128 + row
            for g in range(blocks):
                qpos = orders[pl.ds(me, 1), g:g + 1, :][0] * 128 + col
                at = pl.ds(pl.multiple_of(i * rows + j * 128, 128), 128)
                mask[g, at, :] = jnp.where(kpos <= qpos, 0.0, -1e30).astype(jnp.bfloat16)

    def build_crossed(s):
        def one(i):
            piece(marks, i, 2, me).wait_recv()
            build(i)
        guarded(a - s >= 0, lambda: one(across - 2 * s))
        guarded(jnp.logical_and(s > 0, a + s < line), lambda: one(across + 2 * s))

    open_own(marks)
    early = 2 if line > 2 else 2 * kv_heads
    for p in range(early):
        open_own(p)
    eye[...] = (row == col).astype(jnp.bfloat16)
    build(me)

    def first_head(s, _):
        relay(marks, s)
        step(0, s)
        if kv_heads > 1:
            for p in range(early, 2 * kv_heads):
                guarded(s == min(p - 1, 2), lambda p=p: open_own(p))
        guarded(a - s >= 0, lambda: build(me - 2 * s))
        guarded(a + s < line, lambda: build(me + 2 * s))
        build_crossed(s - 1)
        return 0
    lax.fori_loop(1, line, first_head, 0)
    if kv_heads > 1 and line > 2:
        step(1, 1)
    build_crossed(jnp.int32(line - 1))
    finish(0)
    if kv_heads > 1:
        for s in range(2, line - 1):
            step(1, s)
    q_load.wait()

    chunk = tokens // 4
    factor = math.log2(math.e) / math.sqrt(HEAD_SIZE)
    ones = jnp.ones((chunk, 128), jnp.bfloat16)
    per_block = per_kv // unit

    def attend(h, g, u):
        at = pl.ds(pl.multiple_of(g * 128, 128), 128)
        def head_cols(k):
            return pl.ds(pl.multiple_of((h * per_kv + u * unit + k) * HEAD_SIZE, 128), HEAD_SIZE)
        e = eye[...]
        qa = jnp.concatenate(
            [jnp.concatenate([q[at, head_cols(k)], e], axis=1) for k in range(unit)], axis=0)
        top = None
        for i in range(4):
            ks = pl.ds(i * chunk, chunk)
            ka = jnp.concatenate([kv[2 * h, ks, :], mask[g, ks, :]], axis=1)
            s = lax.dot_general(qa, ka, NT, preferred_element_type=jnp.float32)
            scores[:, ks] = s
            for j in range(0, chunk, 128):
                part = s[:, j:j + 128]
                top = part if top is None else jnp.maximum(top, part)
        top = jnp.max(top, axis=1, keepdims=True)
        acc = None
        for i in range(4):
            ks = pl.ds(i * chunk, chunk)
            weight = jnp.exp2((scores[:, ks] - top) * factor).astype(jnp.bfloat16)
            va = jnp.concatenate([kv[2 * h + 1, ks, :], ones], axis=1)
            part = jnp.dot(weight, va, preferred_element_type=jnp.float32)
            acc = part if acc is None else acc + part
        res = (acc[:, :128] / acc[:, 128:]).astype(jnp.bfloat16)
        for k in range(unit):
            att[at, head_cols(k)] = res[k * 128:(k + 1) * 128]

    total = blocks * per_block
    for h in range(kv_heads):
        def body(i, _):
            attend(h, i // per_block, lax.rem(i, per_block))
            if h == 0 and kv_heads > 1:
                guarded(i == 0, lambda: step(1, line - 1))
            return 0
        lax.fori_loop(0, total, body, 0)
        if h + 1 < kv_heads:
            for s in range(1 if h else line - 1, line) if (h or total < 2) else ():
                step(h + 1, s)
            finish(h + 1)

    quarter = o_ref.shape[1]
    parts = quarter // wide
    w_load.wait()

    def product(group, core, j):
        cols = pl.ds(pl.multiple_of((group * 2 + core) * quarter + j * wide, 128), wide)
        return jnp.dot(att[...], w[:, cols], preferred_element_type=jnp.float32)

    def pair_copy(i, j):
        return pltpu.make_async_remote_copy(
            src_ref=pair_out.at[i, j], dst_ref=pair_in.at[i, j], send_sem=pair_send.at[i, j],
            recv_sem=pair_recv.at[i, j], device_id=partner, device_id_type=MESH)

    def far_copy(i, j):
        return pltpu.make_async_remote_copy(
            src_ref=far_out.at[i, j], dst_ref=far_in.at[i, j], send_sem=far_send.at[i, j],
            recv_sem=far_recv.at[i, j], device_id=(me, far(i) * 2 + c), device_id_type=MESH)

    def far_step(k, _):
        i, j = 1 + k // parts, lax.rem(k, parts)
        pair_out[i, j] = product(far(i), 1 - c, j).astype(jnp.bfloat16)
        pair_copy(i, j).start()
        mine = product(far(i), c, j)
        pair_copy(i, j).wait_recv()
        far_out[i, j] = (mine + pair_in[i, j].astype(jnp.float32)).astype(jnp.bfloat16)
        far_copy(i, j).start()
        return 0
    lax.fori_loop(0, (groups - 1) * parts, far_step, 0)

    def near_step(j, _):
        pair_out[0, j] = product(y, 1 - c, j).astype(jnp.bfloat16)
        pair_copy(0, j).start()
        far_out[0, j] = product(y, c, j).astype(jnp.bfloat16)
        return 0
    lax.fori_loop(0, parts, near_step, 0)

    def close_step(j, _):
        pair_copy(0, j).wait_recv()
        res = far_out[0, j].astype(jnp.float32) + pair_in[0, j].astype(jnp.float32)
        for i in range(1, groups):
            far_copy(i, j).wait_recv()
            res = res + far_in[i, j].astype(jnp.float32)
        o_ref[:, pl.ds(pl.multiple_of(j * wide, 128), wide)] = res.astype(jnp.bfloat16)
        return 0
    lax.fori_loop(0, parts, close_step, 0)

    def drain(i, _):
        for p in range(2 * kv_heads + 1):
            blk = i * 2 + b
            guarded(jnp.logical_and(up, i <= a), lambda: piece(p, blk, 0, me + 2).wait_send())
            guarded(jnp.logical_and(down, i >= a), lambda: piece(p, blk, 1, me - 2).wait_send())
            piece(p, blk, 2, across).wait_send()
        return 0
    lax.fori_loop(0, line, drain, 0)

    def drain_out(j, _):
        for i in range(groups):
            pair_copy(i, j).wait_send()
            if i:
                far_copy(i, j).wait_send()
        return 0
    lax.fori_loop(0, parts, drain_out, 0)


def shards(n, tp, queries, keys, values, out_weight, block_order):
    rows = queries.shape[0]
    heads = queries.shape[1] // HEAD_SIZE
    group = QUERY_HEADS // KEY_VALUE_HEADS
    kv_heads = max(1, heads // group)
    unit = min(4, heads // kv_heads)
    quarter = out_weight.shape[1] // tp
    wide = min(256, quarter)
    parts, groups, tokens, blocks = quarter // wide, tp // 2, n * rows, rows // 128
    dims = (n, tp, rows, heads, kv_heads, unit, wide)
    any_space = pl.BlockSpec(memory_space=pl.ANY)
    dma = pltpu.SemaphoreType.DMA
    bf16 = jnp.bfloat16
    swap = pltpu.VMEM((groups, parts, rows, wide), bf16)
    return pl.pallas_call(
        functools.partial(kernel, dims),
        out_shape=jax.ShapeDtypeStruct((rows, quarter), bf16),
        in_specs=[any_space] * 4 + [pl.BlockSpec(memory_space=pltpu.SMEM)],
        out_specs=pl.BlockSpec(memory_space=pltpu.VMEM),
        scratch_shapes=[
            pltpu.VMEM(queries.shape, bf16),
            pltpu.VMEM(out_weight.shape, bf16),
            pltpu.VMEM((2 * kv_heads, tokens, HEAD_SIZE), bf16),
            pltpu.VMEM((n, 8, 128), jnp.int32),
            pltpu.VMEM((blocks, tokens, 128), bf16),
            pltpu.VMEM((128, 128), bf16),
            pltpu.VMEM((unit * 128, tokens), jnp.float32),
            pltpu.VMEM((rows, heads * HEAD_SIZE), bf16),
            swap, swap, swap, swap,
            dma((2 * kv_heads + 2,)),
            dma((2 * kv_heads + 1, n, 3)), dma((2 * kv_heads + 1, n)),
            dma((groups, parts)), dma((groups, parts)), dma((groups, parts)), dma((groups, parts)),
        ],
        compiler_params=pltpu.CompilerParams(
            collective_id=0, has_side_effects=True, vmem_limit_bytes=60 * 2**20),
    )(queries, keys, values, out_weight, block_order)


def solution(mesh):
    n, tp = mesh.shape["ctx"], mesh.shape["tp"]
    in_specs = (P("ctx", "tp"), P("ctx", None), P("ctx", None), P("tp", None), P("ctx"))
    return jax.shard_map(functools.partial(shards, n, tp), mesh=mesh, in_specs=in_specs,
                         out_specs=P("ctx", "tp"), check_vma=False)
```
